32 devices in a mesh: rows: 8 (over z, y), cols: 4 (over x, core).
Axes of the slice: x: 2, y: 2, z: 4, core: 2. Of those that a mesh axis runs over, the one named last changes fastest.
Arguments:
- slab: float32 [1536, 6144], P('rows', 'cols'), may hold values from -6 to 6
- factor: float32 [6144, 6144], P('cols', 'rows'), may hold values from -0.078125 to 0.078125
- block_inverse: float32 [6144, 1536], P('cols'), may hold values from -2 to 2, as said below
- pivot_order: int32 [6144], replicated, may hold values from 0 to 6143, as said below
- row_count: int32 [8], P('rows'), may hold values from 1 to 192, 1075 in all
Outputs:
- vectors: float32 [1536, 6144], P('rows', 'cols')
- mean_square: float32 [1536], P('rows')
The draws below stay inside these ranges and needn't reach their ends.
Inputs may be any that keep to these rules, and one draw needn't show every extreme that they name: `pivot_order`: each of 0 to 6143 appears once. Of the 1536 pivots of one block, at most 768 have slab columns in any one block of 1536 slab columns, and exactly 768 in some. `row_count`: slots at or beyond the count hold entries that are ignored. `block_inverse`: each block of 1536 rows is lower triangular, with diagonal entries from 0.6 to 1.4.
All inputs are finite; a program needn't handle non-finite values. No bound on the sum of `row_count` on one device may be relied on, other than what follows from the above.
Results may differ from the reference program's by a relative error of at most 0.0001.
Values sent between devices are 32-bit elements; how exact they have to be, the bound alone decides.
No kernel may reach another device: no remote copies, remote signals or barrier semaphores. Data moves between devices by JAX's collectives and lax.ppermute only.
A program may use at most 192 MiB of HBM per device.

```python
import math
import jax
import jax.numpy as jnp
import numpy as np
from jax import lax

K = 6144
ROWS_DEV = 192
BLOCK = 1536
ROWS = 1536
N_ROWS = 8
N_COLS = 4


def draw_block_inverse(key, part):
    first_key, second_key = jax.random.split(key)
    local_rows = jnp.arange(K, dtype=jnp.int32) % BLOCK
    local_cols = jnp.arange(BLOCK, dtype=jnp.int32)
    spread = jnp.clip(jax.random.normal(first_key, (K, BLOCK), jnp.float32), -4.0, 4.0)
    spread = spread / jnp.sqrt(jnp.float32(BLOCK))
    diagonal = jax.random.uniform(second_key, (K, 1), jnp.float32, 0.6, 1.4)
    lower = jnp.where(local_cols[None, :] < local_rows[:, None], spread, jnp.float32(0.0))
    return lower + jnp.where(local_cols[None, :] == local_rows[:, None], diagonal, jnp.float32(0.0))


def draw_pivot_order(key, part):
    keys = jax.random.split(jax.random.fold_in(key, 17), 4)
    group_count = K // BLOCK
    base = BLOCK // group_count
    shift = jax.random.randint(keys[0], (), 0, group_count, dtype=jnp.int32)
    extra = jax.random.randint(keys[1], (), 0, base // 2 + 1, dtype=jnp.int32)
    source = jnp.arange(group_count, dtype=jnp.int32)[:, None]
    target = jnp.arange(group_count, dtype=jnp.int32)[None, :]
    offset = (target - source - shift) % group_count
    counts = base + base * (offset == 0).astype(jnp.int32) - base * (offset == 1).astype(jnp.int32)
    counts = counts + extra * (offset == 2).astype(jnp.int32) - extra * (offset == 3).astype(jnp.int32)
    inclusive = jnp.cumsum(counts, axis=1)
    columns = jnp.arange(K, dtype=jnp.int32)
    column_block = columns // BLOCK
    first_perm = jax.random.permutation(keys[2], K).astype(jnp.int32)
    order = jnp.argsort(column_block * K + first_perm).astype(jnp.int32)
    position = jnp.argsort(order).astype(jnp.int32)
    local_rank = position - column_block * BLOCK
    bounds = jnp.take(inclusive, column_block, axis=0)
    destination = jnp.sum((bounds <= local_rank[:, None]).astype(jnp.int32), axis=1)
    second_perm = jax.random.permutation(keys[3], K).astype(jnp.int32)
    return jnp.argsort(destination * K + second_perm).astype(jnp.int32)


def block_levels(own_key, shape, cuts, least, high):
    def one(axis_at, blocks):
        steps = jax.random.uniform(jax.random.fold_in(jax.random.fold_in(own_key, 6), axis_at), (blocks,), jnp.float32, least / len(cuts), high / len(cuts))
        return jnp.repeat(jnp.exp(steps), shape[axis_at] // blocks).reshape((-1,) + (1,) * (len(shape) - axis_at - 1))

    factor_of = one(*cuts[0])
    for cut in cuts[1:]:
        factor_of = factor_of * one(*cut)
    return factor_of


def length_profile(number_of, total, most, lean):
    loads = [(1 << 20) // math.isqrt(rank ** lean) + 1 for rank in range(2, number_of + 1)]
    surplus, holding = total - most - (number_of - 1), [1] * (number_of - 1)
    while surplus > 0:
        candidates = [i for i in range(number_of - 1) if holding[i] < most]
        mass, remaining = sum([loads[i] for i in candidates]), surplus
        for i in candidates:
            addition = min(most - holding[i], max(1, remaining * loads[i] // mass), surplus)
            holding[i] = holding[i] + addition
            surplus = surplus - addition
    return np.array([most] + holding)


def uneven(stream_key, amount, total, limit, slope):
    if amount == 2:
        one = jax.random.randint(stream_key, (), max(1, total - limit), min(limit, total - 1) + 1)
        return jnp.stack([one, total - one])
    sizes = jnp.asarray(length_profile(amount, total, limit, slope), jnp.int32)
    couples = (amount - 1) // 2
    giver, sink = sizes[1:1 + 2 * couples:2], sizes[2:2 + 2 * couples:2]
    margin = jnp.minimum(giver - 1, limit - sink)
    passed = jax.random.randint(jax.random.fold_in(stream_key, 1), (couples,), 0, 1 << 20) % (margin + 1)
    sizes = sizes.at[1:1 + 2 * couples:2].set(giver - passed).at[2:2 + 2 * couples:2].set(sink + passed)
    return sizes[jax.random.permutation(jax.random.fold_in(stream_key, 2), amount)]


def scatter_about(rng, shape, scale, bound, shards=(), held_as=jnp.bfloat16):
    gain = block_levels(rng, shape, shards, -0.22, 0.18) if shards else 1.0
    drawn = jax.random.normal(rng, shape, jnp.float32) * scale * gain
    return jnp.minimum(jnp.maximum(drawn, -bound), bound).astype(held_as)


def setup_inputs(seed: int = 0) -> dict:
    key_list = jax.random.split(jax.random.key(seed), 6)
    slab = scatter_about(key_list[0], (ROWS, K), 1.0, 6.0, ((0, 8), (1, 4)), jnp.float32)
    factor = scatter_about(key_list[1], (K, K), K ** -0.5, 0.078125, ((0, 4), (1, 8)), jnp.float32)
    block_inverse = draw_block_inverse(jax.random.fold_in(key_list[5], 71), 0)
    pivot_order = draw_pivot_order(jax.random.fold_in(key_list[5], 71), 0)
    row_count = uneven(key_list[4], N_ROWS, (7 * ROWS) // 10, ROWS_DEV, 2).astype(jnp.int32)
    return dict(slab=slab, factor=factor, block_inverse=block_inverse, pivot_order=pivot_order, row_count=row_count)


def reference(slab, factor, block_inverse, pivot_order, row_count):
    ordered = jnp.take(slab, pivot_order, axis=1)
    slot_index = jnp.arange(ROWS, dtype=jnp.int32) % ROWS_DEV
    owner = jnp.arange(ROWS, dtype=jnp.int32) // ROWS_DEV
    live_rows = slot_index < row_count[owner]
    ordered = jnp.where(live_rows[:, None], ordered, jnp.float32(0.0))
    block_width = K // N_COLS
    finished = []
    for column_block in range(N_COLS):
        low = column_block * block_width
        remainder = ordered[:, low:low + block_width]
        for earlier in range(column_block):
            weights = factor[low:low + block_width, earlier * block_width:(earlier + 1) * block_width]
            remainder = remainder - jnp.dot(finished[earlier], weights.T, precision=lax.Precision.HIGHEST, preferred_element_type=jnp.float32)
        inverse = block_inverse[low:low + block_width]
        finished.append(jnp.dot(remainder, inverse.T, precision=lax.Precision.HIGHEST, preferred_element_type=jnp.float32))
    vectors = jnp.concatenate(finished, axis=1)
    mean_square = jnp.sum(vectors * vectors, axis=1) / K
    return vectors, mean_square
```

```python
import functools

import jax
import jax.numpy as jnp
import numpy as np
from jax import lax
from jax.experimental import pallas as pl
from jax.experimental.pallas import tpu as pltpu
from jax.sharding import PartitionSpec as P

AXES = ("rows", "cols")
PARTS = 3
DEPTH = 2
MOVED = 1
CROSS_AT = (3, 5, 10)
PLACES = {
    1: ("cross_1",),
    3: ("swap_sides",),
    6: ("cross_2",),
    7: ("swap_far",),
    8: ("order", "v0"),
    9: ("share_0",),
    12: ("join_0",),
    17: ("stage_0",),
    18: ("v1",),
    19: ("share_1",),
    22: ("join_1",),
}
NEEDS = {
    "cross_1": ("piece_1",),
    "cross_2": ("piece_2",),
    "cross_3": ("piece_3",),
    "swap_sides": ("slab",),
    "swap_far": ("far",),
    "order": ("slab", "near", "far", "far_near"),
    "v0": ("ordered",),
    "share_0": ("v0", "v0_near"),
    "join_0": ("v0", "v0_far"),
    "stage_0": ("v0",),
    "v1": ("ordered", "part", "part_near"),
    "share_1": ("v1", "v1_near"),
    "join_1": ("v1", "v1_far"),
}


def times_transposed(left, right, precision=lax.Precision.HIGH):
    return lax.dot_general(
        left,
        right,
        (((1,), (1,)), ((), ())),
        precision=precision,
        preferred_element_type=jnp.float32,
    )


def ring_schedule(ring_size, source_of, ready, depth):
    have = [dict() for _ in range(ring_size)]
    for chunk, position in source_of.items():
        have[position][chunk] = ready[chunk]
    sent = [set() for _ in range(ring_size)]
    left = len(source_of) * (ring_size - 1)
    rounds = []
    while left:
        now = len(rounds)
        row = [None] * ring_size
        for position in range(ring_size):
            best = None
            for chunk, since in have[position].items():
                source = source_of[chunk]
                if since > now or chunk in sent[position] or (position + 1 - source) % ring_size == 0:
                    continue
                hops_left = ring_size - 1 - (position - source) % ring_size
                key = (chunk[0] > 0, -hops_left, chunk)
                if best is None or key < best[0]:
                    best = (key, chunk)
            if best is not None:
                row[position] = best[1]
        for position, chunk in enumerate(row):
            if chunk is not None:
                sent[position].add(chunk)
                have[(position + 1) % ring_size][chunk] = now + depth
                left -= 1
        rounds.append(row)
    return rounds


HELD = {
    0: {(1, 0): (0, 0, range(PARTS)), (3, 1): (1, PARTS, range(PARTS - MOVED)), (3, 0): (2, 0, range(PARTS))},
    1: {
        (2, 0): (0, 0, range(PARTS)),
        (2, 1): (1, 0, range(PARTS)),
        (3, 1): (1, MOVED, range(PARTS - MOVED, PARTS)),
        (3, 2): (2, 0, range(PARTS)),
    },
}
SIZES = (PARTS, PARTS + max(MOVED, PARTS - MOVED), PARTS)
STARTS = (0, 2 * SIZES[0], 2 * (SIZES[0] + SIZES[1]))
SPARE = 2 * sum(SIZES)


def slot_of(chunk):
    stage, place, piece = chunk
    return STARTS[stage] + piece * SIZES[stage] + place


def copy(source, target, sem):
    return pltpu.make_async_copy(source, target, sem)


def bits_at(values, index):
    found = jnp.int32(0)
    for bit in range(int(max(values)).bit_length()):
        word = sum(((int(value) >> bit) & 1) << place for place, value in enumerate(values))
        if word:
            word = np.int32(word - (1 << 32) if word >= 1 << 31 else word)
            found = found | ((lax.shift_right_logical(word, index) & 1) << bit)
    return found


ANYWHERE = pl.BlockSpec(memory_space=pl.ANY)


def kernel(body, name, operands, out_shape, scratch, aliases=None):
    return pl.pallas_call(
        body,
        out_shape=out_shape,
        grid_spec=pltpu.PrefetchScalarGridSpec(
            num_scalar_prefetch=1,
            grid=(),
            in_specs=[ANYWHERE] * (len(operands) - 1),
            out_specs=[ANYWHERE] * len(out_shape),
            scratch_shapes=scratch,
        ),
        input_output_aliases=aliases or {},
        name=name,
    )(*operands)


def other_half(device, factor, half):
    def body(device_ref, factor_ref, out_ref, stage, sem):
        low = pl.multiple_of((device_ref[0] & 1) * half, half)
        for step in (copy(factor_ref.at[pl.ds(low, half)], stage, sem), copy(stage, out_ref, sem)):
            step.start()
            step.wait()

    shape = (half, factor.shape[1])
    return kernel(
        body,
        "other_half",
        (device, factor),
        [jax.ShapeDtypeStruct(shape, factor.dtype)],
        [pltpu.VMEM(shape, factor.dtype), pltpu.SemaphoreType.DMA],
    )[0]


def first_chunks(device, factor, yours, own, other, half, chunk_rows):
    columns = factor.shape[1]

    def body(device_ref, factor_ref, yours_ref, store_ref, *rest):
        cross_refs, stage, sems = rest[:PARTS], rest[PARTS], rest[PARTS + 1]
        here = device_ref[0]
        low = pl.multiple_of((1 - (here & 1)) * half, half)
        mine = copy(factor_ref.at[pl.ds(low, half)], stage.at[0], sems.at[0])
        theirs = copy(yours_ref, stage.at[1], sems.at[1])
        mine.start()
        theirs.start()
        carrier = 1 - (here & 1)
        out = []
        for which, (load, table) in enumerate(((mine, own), (theirs, other))):
            load.wait()
            for part in range(PARTS):
                slot = bits_at(table[part], here)
                piece = stage.at[which, pl.ds(part * chunk_rows, chunk_rows)]
                out.append((slot != SPARE, copy(piece, store_ref.at[slot], sems.at[2 + which * PARTS + part])))
                out.append((carrier == which, copy(piece, cross_refs[part], sems.at[2 + 2 * PARTS + part])))
            for wanted, move in out[-2 * PARTS :]:
                pl.when(wanted)(move.start)
        for wanted, move in out:
            pl.when(wanted)(move.wait)

    chunk = jax.ShapeDtypeStruct((chunk_rows, columns), factor.dtype)
    return kernel(
        body,
        "first_chunks",
        (device, factor, yours),
        [jax.ShapeDtypeStruct((SPARE, chunk_rows, columns), factor.dtype)] + [chunk] * PARTS,
        [pltpu.VMEM((2, half, columns), factor.dtype), pltpu.SemaphoreType.DMA((2 + 3 * PARTS,))],
    )


def hop(device, store, arrivals, tables, send_table):
    count = len(arrivals)
    sends = send_table is not None
    chunk_shape = store.shape[1:]

    def body(device_ref, *refs):
        arrival_refs, store_ref = refs[1 : 1 + count], refs[1 + count]
        stage, loads, stores, last = refs[-4:]
        here = device_ref[0]
        slots = [bits_at(table, here) for table in tables]
        kept = [slot != SPARE for slot in slots]
        pull = [copy(arrival_refs[i], stage.at[i], loads.at[i]) for i in range(count)]
        push = [copy(stage.at[i], store_ref.at[slots[i]], stores.at[i]) for i in range(count)]
        for i in range(count):
            pl.when(kept[i])(pull[i].start)
        if sends:
            send_ref = refs[2 + count]
            send_slot = bits_at(send_table, here)
            sending = send_slot != SPARE
            stored = sending
            for slot in slots:
                stored = stored & (slot != send_slot)
            fetch = copy(store_ref.at[send_slot], stage.at[count], loads.at[count])
            pl.when(stored)(fetch.start)
            give = [copy(stage.at[i], send_ref, last) for i in range(count + 1)]
        for i in range(count):
            pl.when(kept[i])(pull[i].wait)
            pl.when(kept[i])(push[i].start)
            if sends:
                pl.when(kept[i] & (slots[i] == send_slot))(give[i].start)
        if sends:

            @pl.when(stored)
            def _():
                fetch.wait()
                give[count].start()

            pl.when(sending)(give[count].wait)
        for i in range(count):
            pl.when(kept[i])(push[i].wait)

    out_shape = [jax.ShapeDtypeStruct(store.shape, store.dtype)]
    if sends:
        out_shape.append(jax.ShapeDtypeStruct(chunk_shape, store.dtype))
    out = kernel(
        body,
        "hop",
        (device, store, *arrivals),
        out_shape,
        [
            pltpu.VMEM((count + 1, *chunk_shape), store.dtype),
            pltpu.SemaphoreType.DMA((count + 1,)),
            pltpu.SemaphoreType.DMA((count + 1,)),
            pltpu.SemaphoreType.DMA,
        ],
        {1: 0},
    )
    return out if sends else (out[0], None)


def side_by_side(device, pieces):
    rows, width = pieces[0].shape
    count = len(pieces)

    def body(device_ref, *refs):
        pieces_in, out_ref, stage, sems = refs[:count], refs[count], refs[count + 1], refs[count + 2]
        places = [pl.ds(i * width, width) for i in range(count)]
        pull = [copy(pieces_in[i], stage.at[:, places[i]], sems.at[i]) for i in range(count)]
        push = [copy(stage.at[:, places[i]], out_ref.at[:, places[i]], sems.at[count + i]) for i in range(count)]
        for move in pull:
            move.start()
        for i in range(count):
            pull[i].wait()
            push[i].start()
        for move in push:
            move.wait()

    shape = (rows, width * count)
    return kernel(
        body,
        "side_by_side",
        (device, *pieces),
        [jax.ShapeDtypeStruct(shape, pieces[0].dtype)],
        [pltpu.VMEM(shape, pieces[0].dtype), pltpu.SemaphoreType.DMA((2 * count,))],
    )[0]


@functools.lru_cache(maxsize=None)
def plan(row_count):
    order = list(range(0, row_count, 2)) + list(range(row_count - 1, 0, -2))
    rounds = {}
    for side in range(2):
        for core in range(2):
            ring = order if core == 1 else order[::-1]
            source_of, ready = {}, {}
            for (block, earlier), (stage, base, parts) in HELD[side].items():
                for part in parts:
                    for piece in range(2):
                        chunk = (stage, base + part, piece)
                        source_of[chunk] = ring.index(earlier * 2 + piece)
                        ready[chunk] = CROSS_AT[part] if side == 0 and block == 3 else 0
            rounds[side, core] = (ring, ring_schedule(row_count, source_of, ready, DEPTH))
    total = max(len(steps) for _, steps in rounds.values())
    send = np.full((total, row_count * 4), SPARE, np.int32)
    arrive = np.full((total, row_count * 4), SPARE, np.int32)
    pairs = [[] for _ in range(total)]
    last = [0, 0, 0]
    for (side, core), (ring, steps) in rounds.items():
        column = side * 2 + core
        for step, row in enumerate(steps):
            for position, chunk in enumerate(row):
                if chunk is None:
                    continue
                here = ring[position] * 4 + column
                there = ring[(position + 1) % row_count] * 4 + column
                send[step, here] = slot_of(chunk)
                arrive[step, there] = slot_of(chunk)
                pairs[step].append((here, there))
                last[chunk[0]] = max(last[chunk[0]], step)
    own = np.full((PARTS, row_count * 4), SPARE, np.int32)
    other = np.full((PARTS, row_count * 4), SPARE, np.int32)
    cross = np.full((PARTS, row_count * 4), SPARE, np.int32)
    for row in range(row_count):
        earlier, piece = row // 2, row % 2
        for column in range(4):
            side = column // 2
            here = row * 4 + column
            for table, block in ((own, column), (other, column ^ 1)):
                if (block, earlier) in HELD[side] and block // 2 == side:
                    stage, base, parts = HELD[side][block, earlier]
                    for part in parts:
                        table[part, here] = slot_of((stage, base + part, piece))
            if side == 0 and (3, earlier) in HELD[0]:
                stage, base, parts = HELD[0][3, earlier]
                for part in parts:
                    cross[part, here] = slot_of((stage, base + part, piece))
    crossing = []
    for part in range(PARTS):
        rows = [r for r in range(row_count) if (3, r // 2) in HELD[0] and part in HELD[0][3, r // 2][2]]
        crossing.append([(r * 4 + 2 + core, r * 4 + core) for r in rows for core in range(2)])
    return send, arrive, pairs, own, other, cross, crossing, last


def ringed(slab, factor, block_inverse, pivot_order, row_count, *, sizes):
    row_indices, column_count = sizes
    rows_here, width = slab.shape
    half = width // 2
    chunk_rows = half // PARTS
    total_width = width * column_count
    row = lax.axis_index("rows")
    column = lax.axis_index("cols")
    core = column % 2
    side = column // 2
    here = row * column_count + column
    send, arrive, pairs, own, other, cross, crossing, last = plan(row_indices)
    steps = len(pairs)
    device = here.astype(jnp.int32)[None]

    everyone = [(r, c) for r in range(row_indices) for c in range(column_count)]

    def move(value, of):
        found = [(r * column_count + c, r * column_count + of(c)) for r, c in everyone if of(c) is not None]
        return lax.ppermute(value, AXES, found)

    def swap_core(value):
        return move(value, lambda c: c ^ 1)

    def swap_side(value):
        return move(value, lambda c: c ^ 2)

    is_core = core == 1
    is_far = side == 1
    yours = swap_core(other_half(device, factor, half))
    store, *pieces = first_chunks(device, factor, yours, own, other, half, chunk_rows)
    state = {"slab": slab, "near": swap_core(slab)}
    state.update({f"piece_{part}": pieces[part] for part in range(1, PARTS)})
    state["cross_0"] = lax.ppermute(pieces[0], AXES, crossing[0])

    def order_columns(values):
        chosen = lax.dynamic_slice_in_dim(pivot_order, column * width, width)
        slot = (chosen // width) ^ column
        slabs = side_by_side(device, values)
        ordered = jnp.take(slabs, slot * width + chosen % width, axis=1)
        live_rows = jnp.arange(rows_here, dtype=jnp.int32) < row_count[0]
        return jnp.where(live_rows[:, None], ordered, jnp.float32(0.0))

    def finish(which, remainder, before=None):
        def idle(values):
            return jnp.zeros_like(values) if before is None else before

        return lax.cond(column == which, lambda r: times_transposed(r, block_inverse), idle, remainder)

    def cross_over(vectors):
        part = rows_here // 2
        piece = lax.dynamic_slice_in_dim(vectors, core * part, part)
        arrived = move(piece, lambda c: {0: 2, 1: 3}.get(c))
        return arrived

    def join_rows(arrived, vectors):
        neighbour = swap_core(arrived)
        whole = jnp.concatenate([jnp.where(is_core, neighbour, arrived), jnp.where(is_core, arrived, neighbour)], axis=0)
        return jnp.where(is_far, whole, vectors)

    def product(vectors, store, stage):
        low, count = STARTS[stage], SIZES[stage]
        total = None
        for piece in range(2):
            weights = store[low + piece * count : low + (piece + 1) * count].reshape(count * chunk_rows, half)
            term = times_transposed(vectors[:, piece * half : (piece + 1) * half], weights)
            total = term if total is None else total + term
        return total

    def both_halves(mine, yours):
        return jnp.concatenate([jnp.where(is_core, mine, yours), jnp.where(is_core, yours, mine)], axis=1)

    def send_cross(part):
        def task(store):
            state[f"cross_{part}"] = lax.ppermute(state.pop(f"piece_{part}"), AXES, crossing[part])

        return task

    def swap_sides(store):
        state["far"] = swap_side(state["slab"])

    def swap_far(store):
        state["far_near"] = swap_core(state["far"])

    def order(store):
        state["ordered"] = order_columns([state.pop(name) for name in ("slab", "near", "far", "far_near")])
        return state["ordered"]

    def first_finish(store):
        state["v0"] = finish(0, state["ordered"])
        state["v0_near"] = move(state["v0"], lambda c: {0: 1}.get(c))
        return state["v0"]

    def stage_0(store):
        state["part"] = product(state["v0"], store, 0)
        state["part_near"] = swap_core(state["part"])
        return state["part"]

    def second_finish(store):
        state["pending"] = state["ordered"] - both_halves(state.pop("part"), state.pop("part_near"))
        state["v1"] = finish(1, state["pending"])
        state["v1_near"] = move(state["v1"], lambda c: {1: 0}.get(c))
        return state["v1"]

    def share(name):
        def task(store):
            state[name] = state[name] + state.pop(name + "_near")
            state[name + "_far"] = cross_over(state[name])
            return state[name]

        return task

    def join(name):
        def task(store):
            state[name] = join_rows(state.pop(name + "_far"), state[name])
            return state[name]

        return task

    tasks = {
        "swap_sides": swap_sides,
        "swap_far": swap_far,
        "order": order,
        "v0": first_finish,
        "share_0": share("v0"),
        "join_0": join("v0"),
        "stage_0": stage_0,
        "v1": second_finish,
        "share_1": share("v1"),
        "join_1": join("v1"),
        **{f"cross_{part}": send_cross(part) for part in range(1, PARTS)},
    }

    def run_tasks(step, store):
        for name in PLACES.get(step, ()):
            keys = [key for key in state if key in NEEDS[name]]
            store, tied = lax.optimization_barrier((store, [state[key] for key in keys]))
            state.update(zip(keys, tied))
            result = tasks[name](store)
            if result is not None:
                store, _ = lax.optimization_barrier((store, result))
        return store

    arrived = [None] * steps
    for step in range(steps + DEPTH):
        values, tables = [], []
        if step >= DEPTH:
            values.append(arrived[step - DEPTH])
            tables.append(arrive[step - DEPTH])
        for part in range(PARTS):
            if CROSS_AT[part] == step:
                values.append(state.pop(f"cross_{part}"))
                tables.append(cross[part])
        store, outgoing = hop(device, store, values, tables, send[step] if step < steps else None)
        if step < steps:
            arrived[step] = lax.ppermute(outgoing, AXES, pairs[step])
        store = run_tasks(step, store)

    part_2 = product(state["v1"], store, 1)
    part_3a = product(state["v0"], store, 2)
    extra = part_2[:, half:]
    low = (PARTS - MOVED) * chunk_rows
    empty = jnp.zeros((rows_here, half), jnp.float32)
    extra_first = jnp.concatenate([extra[:, :low], empty[:, low:]], axis=1)
    extra_last = jnp.concatenate([empty[:, :low], extra[:, : half - low]], axis=1)
    carried = move(part_3a + extra_first, lambda c: {0: 2, 1: 3}.get(c))
    part_2_main = part_2[:, :half]
    pending = state["pending"] - both_halves(part_2_main, swap_core(part_2_main))
    third = finish(2, pending)
    shared_2 = third + move(third, lambda c: {2: 3}.get(c))
    part_3b = product(shared_2, store, 2)
    part_3 = part_3b + carried + extra_last
    last_pending = state["ordered"] - both_halves(part_3, swap_core(part_3))
    first = jnp.where(column == 0, state["v0"], state["v1"])
    vectors = finish(3, last_pending, jnp.where(is_far, third, first))
    row_sums = lax.psum(jnp.sum(vectors * vectors, axis=1), "cols")
    return (vectors, row_sums / total_width)


def gathered(slab, factor, block_inverse, pivot_order, row_count):
    rows_here = slab.shape[0]
    block_width = slab.shape[1]
    column_count = lax.axis_size("cols")
    column = lax.axis_index("cols")
    total_width = block_width * column_count
    chosen = lax.dynamic_slice_in_dim(pivot_order, column * block_width, block_width)
    everything = lax.all_gather(slab, "cols", axis=1, tiled=True)
    ordered = jnp.take(everything, chosen, axis=1)
    live_rows = jnp.arange(rows_here, dtype=jnp.int32) < row_count[0]
    ordered = jnp.where(live_rows[:, None], ordered, jnp.float32(0.0))
    factor_row = lax.all_gather(factor, "rows", axis=1, tiled=True)

    def finish(values):
        return times_transposed(values, block_inverse)

    pending = ordered
    vectors = jnp.zeros_like(ordered)
    for column_block in range(column_count):
        finished = lax.cond(column == column_block, finish, jnp.zeros_like, pending)
        vectors = vectors + finished
        if column_block + 1 < column_count:
            arrived = lax.psum(finished, "cols")
            weights = factor_row[:, column_block * block_width : (column_block + 1) * block_width]
            update = times_transposed(arrived, weights)
            pending = pending - jnp.where(column_block < column, update, jnp.float32(0.0))
    row_sums = lax.psum(jnp.sum(vectors * vectors, axis=1), "cols")
    return (vectors, row_sums / total_width)


def solution(mesh):
    placed = (P("rows", "cols"), P("cols", "rows"), P("cols", None), P(), P("rows"))
    row_indices, column_count = mesh.shape["rows"], mesh.shape["cols"]
    if row_indices == 2 * column_count and column_count == 4:
        work = functools.partial(ringed, sizes=(row_indices, column_count))
    else:
        work = gathered
    return jax.shard_map(
        work,
        mesh=mesh,
        in_specs=placed,
        out_specs=(P("rows", "cols"), P("rows")),
        check_vma=False,
    )
```

```python
import functools
import types

import jax
import jax.numpy as jnp
import numpy as np
from jax import lax
from jax.experimental import pallas as pl
from jax.experimental.pallas import tpu as pltpu
from jax.sharding import PartitionSpec as P


AXES = ("rows", "cols")
PARTS = 3
DEPTH = 2
TILES = 6
MOVED = 2
CROSS_AT = (5, 7, 9)
CROSS_SENT = (0, 0, 1)
SWAP_FAR, ORDER, V0, PASS_0 = 3, 4, 6, 10
STAGE_0, V1, PASS_1, STAGE_1, V2, CARRY = 17, 18, 21, 22, 24, 24
BIAS = {(1, 1, 0): 2.0, (1, 2, 0): 0.9}


def times_transposed(left, right, precision=lax.Precision.HIGH):
    return lax.dot_general(
        left,
        right,
        (((1,), (1,)), ((), ())),
        precision=precision,
        preferred_element_type=jnp.float32,
    )


def ring_schedule(ring_size, source_of, ready, bias, depth):
    have = [dict() for _ in range(ring_size)]
    for chunk, position in source_of.items():
        have[position][chunk] = ready[chunk]
    sent = [set() for _ in range(ring_size)]
    left = len(source_of) * (ring_size - 1)
    rounds = []
    while left:
        now = len(rounds)
        row = [None] * ring_size
        for position in range(ring_size):
            best = None
            for chunk, since in have[position].items():
                source = source_of[chunk]
                if since > now or chunk in sent[position] or (position + 1 - source) % ring_size == 0:
                    continue
                hops_left = ring_size - 1 - (position - source) % ring_size
                key = (chunk[0] > 0, -hops_left - bias[chunk], chunk)
                if best is None or key < best[0]:
                    best = (key, chunk)
            if best is not None:
                row[position] = best[1]
        for position, chunk in enumerate(row):
            if chunk is not None:
                sent[position].add(chunk)
                have[(position + 1) % ring_size][chunk] = now + depth
                left -= 1
        rounds.append(row)
    return rounds


HELD = {
    0: {(1, 0): (0, 0, range(PARTS)), (3, 1): (1, PARTS, range(PARTS - MOVED)), (3, 0): (2, 0, range(PARTS))},
    1: {
        (2, 0): (0, 0, range(PARTS)),
        (2, 1): (1, 0, range(PARTS)),
        (3, 1): (1, MOVED, range(PARTS - MOVED, PARTS)),
        (3, 2): (2, 0, range(PARTS)),
    },
}
SIZES = (PARTS, PARTS + max(MOVED, PARTS - MOVED), PARTS)
STARTS = (0, 2 * SIZES[0], 2 * (SIZES[0] + SIZES[1]))
SPARE = 2 * sum(SIZES)


def slot_of(chunk):
    stage, place, piece = chunk
    return STARTS[stage] + piece * SIZES[stage] + place


def copy(source, target, sem):
    return pltpu.make_async_copy(source, target, sem)


def bits_at(values, index):
    found = jnp.int32(0)
    for bit in range(int(max(values)).bit_length()):
        word = sum(((int(value) >> bit) & 1) << place for place, value in enumerate(values))
        if word:
            word = np.int32(word - (1 << 32) if word >= 1 << 31 else word)
            found = found | ((lax.shift_right_logical(word, index) & 1) << bit)
    return found


ANYWHERE = pl.BlockSpec(memory_space=pl.ANY)


def kernel(body, operands, out_shape, scratch, aliases=None):
    return pl.pallas_call(
        body,
        out_shape=out_shape,
        grid_spec=pltpu.PrefetchScalarGridSpec(
            num_scalar_prefetch=1,
            grid=(),
            in_specs=[ANYWHERE] * (len(operands) - 1),
            out_specs=[ANYWHERE] * len(out_shape),
            scratch_shapes=scratch,
        ),
        input_output_aliases=aliases or {},
    )(*operands)


def other_half(device, factor, half):
    def body(device_ref, factor_ref, out_ref, stage, sem):
        low = pl.multiple_of((device_ref[0] & 1) * half, half)
        for step in (copy(factor_ref.at[pl.ds(low, half)], stage, sem), copy(stage, out_ref, sem)):
            step.start()
            step.wait()

    shape = (half, factor.shape[1])
    return kernel(
        body,
        (device, factor),
        [jax.ShapeDtypeStruct(shape, factor.dtype)],
        [pltpu.VMEM(shape, factor.dtype), pltpu.SemaphoreType.DMA],
    )[0]


def first_chunks(device, factor, yours, own, other, half, chunk_rows):
    columns = factor.shape[1]

    def body(device_ref, factor_ref, yours_ref, store_ref, *rest):
        cross_refs, stage, sems = rest[:PARTS], rest[PARTS], rest[PARTS + 1]
        here = device_ref[0]
        low = pl.multiple_of((1 - (here & 1)) * half, half)
        mine = copy(factor_ref.at[pl.ds(low, half)], stage.at[0], sems.at[0])
        theirs = copy(yours_ref, stage.at[1], sems.at[1])
        mine.start()
        theirs.start()
        carrier = 1 - (here & 1)
        out = []
        for which, (load, table) in enumerate(((mine, own), (theirs, other))):
            load.wait()
            for part in range(PARTS):
                slot = bits_at(table[part], here)
                piece = stage.at[which, pl.ds(part * chunk_rows, chunk_rows)]
                out.append((slot != SPARE, copy(piece, store_ref.at[slot], sems.at[2 + which * PARTS + part])))
                out.append((carrier == which, copy(piece, cross_refs[part], sems.at[2 + 2 * PARTS + part])))
            for wanted, move in out[-2 * PARTS :]:
                pl.when(wanted)(move.start)
        for wanted, move in out:
            pl.when(wanted)(move.wait)

    chunk = jax.ShapeDtypeStruct((chunk_rows, columns), factor.dtype)
    return kernel(
        body,
        (device, factor, yours),
        [jax.ShapeDtypeStruct((SPARE, chunk_rows, columns), factor.dtype)] + [chunk] * PARTS,
        [pltpu.VMEM((2, half, columns), factor.dtype), pltpu.SemaphoreType.DMA((2 + 3 * PARTS,))],
    )


def hop(device, store, arrivals, tables, send_table):
    count = len(arrivals)
    sends = send_table is not None
    chunk_shape = store.shape[1:]

    def body(device_ref, *refs):
        arrival_refs, store_ref = refs[1 : 1 + count], refs[1 + count]
        stage, loads, stores, last = refs[-4:]
        here = device_ref[0]
        slots = [bits_at(table, here) for table in tables]
        kept = [slot != SPARE for slot in slots]
        pull = [copy(arrival_refs[i], stage.at[i], loads.at[i]) for i in range(count)]
        push = [copy(stage.at[i], store_ref.at[slots[i]], stores.at[i]) for i in range(count)]
        for i in range(count):
            pl.when(kept[i])(pull[i].start)
        if sends:
            send_ref = refs[2 + count]
            send_slot = bits_at(send_table, here)
            sending = send_slot != SPARE
            stored = sending
            for slot in slots:
                stored = stored & (slot != send_slot)
            fetch = copy(store_ref.at[send_slot], stage.at[count], loads.at[count])
            pl.when(stored)(fetch.start)
            give = [copy(stage.at[i], send_ref, last) for i in range(count + 1)]
        for i in range(count):
            pl.when(kept[i])(pull[i].wait)
            pl.when(kept[i])(push[i].start)
            if sends:
                pl.when(kept[i] & (slots[i] == send_slot))(give[i].start)
        if sends:

            @pl.when(stored)
            def _():
                fetch.wait()
                give[count].start()

            pl.when(sending)(give[count].wait)
        for i in range(count):
            pl.when(kept[i])(push[i].wait)

    out_shape = [jax.ShapeDtypeStruct(store.shape, store.dtype)]
    if sends:
        out_shape.append(jax.ShapeDtypeStruct(chunk_shape, store.dtype))
    out = kernel(
        body,
        (device, store, *arrivals),
        out_shape,
        [
            pltpu.VMEM((count + 1, *chunk_shape), store.dtype),
            pltpu.SemaphoreType.DMA((count + 1,)),
            pltpu.SemaphoreType.DMA((count + 1,)),
            pltpu.SemaphoreType.DMA,
        ],
        {1: 0},
    )
    return out if sends else (out[0], None)


def parts_of(value):
    high = value.astype(jnp.bfloat16)
    return high, (value - high.astype(jnp.float32)).astype(jnp.bfloat16)


def padded(rows):
    return -(-rows // 256) * 256


def three_passes(weights, left):
    high, low = parts_of(weights)
    return lax.dot_general(
        jnp.concatenate([high, high, low], axis=1),
        jnp.concatenate([left[0], left[1], left[0]], axis=1),
        (((1,), (1,)), ((), ())),
        preferred_element_type=jnp.float32,
    )


def product(device, store, terms, side=None, addend=None):
    rows, width = next(iter(terms[0][0].values())).shape
    chunk_rows, half = store.shape[1:]
    chunks = terms[0][3]
    most = sum(term[3] for term in terms)
    arrays = [array for term in terms for array in term[0].values()] + ([] if addend is None else [addend])

    def body(device_ref, store_ref, *rest):
        array_refs, (out_ref, left, weights, out, sems) = rest[: len(arrays)], rest[len(arrays) :]
        column = device_ref[0] & 3

        def work():
            pulls, loads, start, given = [], [], 0, 0
            for t, (vectors, low, stride, count, _) in enumerate(terms):
                pulls.append([])
                for holder in vectors:
                    pull = copy(array_refs[given], left.at[t, pl.ds(0, rows)], sems.at[2 * most + t])
                    pulls[-1].append((column == holder, pull))
                    pl.when(column == holder)(pull.start)
                    given += 1
                for piece in range(2):
                    loads.append([])
                    for i in range(count):
                        place = weights.at[piece, pl.ds((start + i) * chunk_rows, chunk_rows)]
                        load = copy(store_ref.at[low + piece * stride + i], place, sems.at[2 * (start + i) + piece])
                        load.start()
                        loads[-1].append(load)
                start += count
            base = []
            if addend is not None:
                base = [copy(array_refs[-1], out, sems.at[2 * most + len(terms)])]
                base[0].start()
            start = 0
            for t, (_, _, _, count, first) in enumerate(terms):
                for wanted, pull in pulls[t]:
                    pl.when(wanted)(pull.wait)
                total = None
                for piece in range(2):
                    parts = parts_of(left[t, :, piece * half : (piece + 1) * half])
                    for load in loads[2 * t + piece]:
                        load.wait()
                    used = weights[piece, start * chunk_rows : (start + count) * chunk_rows]
                    term = three_passes(used, parts)
                    total = term if total is None else total + term
                for load in base if t == 0 else []:
                    load.wait()
                place = slice(first * chunk_rows, (first + count) * chunk_rows)
                turned = total.T[:rows]
                out[:, place] = out[:, place] + turned if t or base else turned
                start += count
            push = copy(out, out_ref, sems.at[0])
            push.start()
            push.wait()

        if side is None:
            work()
        else:
            pl.when((column >> 1) == side)(work)

    return kernel(
        body,
        (device, store, *arrays),
        [jax.ShapeDtypeStruct((rows, chunks * chunk_rows), jnp.float32)],
        [
            pltpu.VMEM((len(terms), padded(rows), width), jnp.float32),
            pltpu.VMEM((2, most * chunk_rows, half), jnp.float32),
            pltpu.VMEM((rows, chunks * chunk_rows), jnp.float32),
            pltpu.SemaphoreType.DMA((2 * most + len(terms) + 1,)),
        ],
    )[0]


def finish(device, which, ordered, block_inverse, updates=(), before=None):
    rows, width = ordered.shape
    half = width // 2
    tile = width // TILES
    pieces = [piece for update in updates for piece in update]
    before = before or {}
    more = pieces + list(before.values())

    def body(device_ref, ordered_ref, inverse_ref, *rest):
        more_refs, (out_ref, left, less, weights, turned, out, sems) = rest[: len(more)], rest[len(more) :]
        here = device_ref[0] & 3

        @pl.when(here == which)
        def _():
            loads = []
            for i in range(TILES):
                place = (pl.ds(i * tile, width - i * tile), pl.ds(i * tile, tile))
                loads.append(copy(inverse_ref.at[place], weights.at[place], sems.at[i]))
            pulls = [copy(ordered_ref, left.at[pl.ds(0, rows)], sems.at[TILES])]
            for i in range(len(pieces)):
                pulls.append(copy(more_refs[i], less.at[i], sems.at[TILES + 1 + i]))
            for move in pulls + loads:
                move.start()
            for move in pulls:
                move.wait()
            for i in range(len(pieces)):
                place = slice((i % 2) * half, (i % 2 + 1) * half)
                left[:rows, place] = left[:rows, place] - less[i]
            for i in range(TILES):
                low = i * tile
                loads[i].wait()
                term = three_passes(weights[low:, low : low + tile], parts_of(left[:, low : low + tile]))
                turned[low:] = term if i == 0 else turned[low:] + term
            for i in range(TILES):
                out[:, i * tile : (i + 1) * tile] = turned[i * tile : (i + 1) * tile].T[:rows]
            push = copy(out, out_ref, sems.at[0])
            push.start()
            push.wait()

        @pl.when(here != which)
        def _():
            if not before:
                out[...] = jnp.zeros_like(out)
            for held, ref in zip(before, more_refs[len(pieces) :]):

                @pl.when(here == held)
                def _():
                    pull = copy(ref, out, sems.at[1])
                    pull.start()
                    pull.wait()

            push = copy(out, out_ref, sems.at[0])
            push.start()
            push.wait()

    return kernel(
        body,
        (device, ordered, block_inverse, *more),
        [jax.ShapeDtypeStruct((rows, width), jnp.float32)],
        [
            pltpu.VMEM((padded(rows), width), jnp.float32),
            pltpu.VMEM((max(1, len(pieces)), rows, half), jnp.float32),
            pltpu.VMEM((width, width), jnp.float32),
            pltpu.VMEM((width, padded(rows)), jnp.float32),
            pltpu.VMEM((rows, width), jnp.float32),
            pltpu.SemaphoreType.DMA((TILES + 1 + len(pieces),)),
        ],
    )[0]


def pick_columns(device, index, live, pieces):
    rows, width = pieces[0].shape
    count = len(pieces)
    tall = padded(rows)

    def body(device_ref, index_ref, live_ref, *refs):
        piece_refs, (out_ref, stage, turned, got, out, sems) = refs[:count], refs[count:]
        pulls = [copy(piece_refs[i], stage.at[i, pl.ds(0, rows)], sems.at[i]) for i in range(count)]
        for pull in pulls:
            pull.start()
        for i in range(count):
            pulls[i].wait()
            turned[i * width : (i + 1) * width] = stage[i].T

        def eight(group, carry):
            start = pl.multiple_of(group * 8, 8)
            lines = [turned[pl.ds(index_ref[start + line], 1), :] for line in range(8)]
            got[pl.ds(start, 8), :] = jnp.concatenate(lines, axis=0)
            return carry

        lax.fori_loop(0, width // 8, eight, 0, unroll=4)
        kept = lax.broadcasted_iota(jnp.int32, (rows, width), 0) < live_ref[0]
        out[...] = jnp.where(kept, got[...].T[:rows], jnp.float32(0.0))
        push = copy(out, out_ref, sems.at[0])
        push.start()
        push.wait()

    return pl.pallas_call(
        body,
        out_shape=jax.ShapeDtypeStruct((rows, width), jnp.float32),
        grid_spec=pltpu.PrefetchScalarGridSpec(
            num_scalar_prefetch=3,
            grid=(),
            in_specs=[ANYWHERE] * count,
            out_specs=ANYWHERE,
            scratch_shapes=[
                pltpu.VMEM((count, tall, width), jnp.float32),
                pltpu.VMEM((count * width, tall), jnp.float32),
                pltpu.VMEM((width, tall), jnp.float32),
                pltpu.VMEM((rows, width), jnp.float32),
                pltpu.SemaphoreType.DMA((count,)),
            ],
        ),
        name="pick_columns",
    )(device, index, live, *pieces)


@functools.lru_cache(maxsize=None)
def plan(row_count):
    order = list(range(0, row_count, 2)) + list(range(row_count - 1, 0, -2))
    rounds = {}
    for side in range(2):
        for core in range(2):
            ring = order if core == 1 else order[::-1]
            source_of, ready, bias = {}, {}, {}
            for (block, earlier), (stage, base, parts) in HELD[side].items():
                for part in parts:
                    for piece in range(2):
                        chunk = (stage, base + part, piece)
                        source_of[chunk] = ring.index(earlier * 2 + piece)
                        bias[chunk] = BIAS.get((side, stage, int(stage == 1 and base + part >= PARTS)), 0.0)
                        ready[chunk] = CROSS_AT[part] if side == 0 and block == 3 else 0
            rounds[side, core] = (ring, ring_schedule(row_count, source_of, ready, bias, DEPTH))
    total = max(len(steps) for _, steps in rounds.values())
    send = np.full((total, row_count * 4), SPARE, np.int32)
    arrive = np.full((total, row_count * 4), SPARE, np.int32)
    pairs = [[] for _ in range(total)]
    last = {}
    for (side, core), (ring, steps) in rounds.items():
        column = side * 2 + core
        for step, row in enumerate(steps):
            for position, chunk in enumerate(row):
                if chunk is None:
                    continue
                here = ring[position] * 4 + column
                there = ring[(position + 1) % row_count] * 4 + column
                send[step, here] = slot_of(chunk)
                arrive[step, there] = slot_of(chunk)
                pairs[step].append((here, there))
                kind = (side, chunk[0], int(chunk[0] == 1 and chunk[1] >= PARTS))
                last[kind] = max(last.get(kind, 0), step)
    own = np.full((PARTS, row_count * 4), SPARE, np.int32)
    other = np.full((PARTS, row_count * 4), SPARE, np.int32)
    cross = np.full((PARTS, row_count * 4), SPARE, np.int32)
    for row in range(row_count):
        earlier, piece = row // 2, row % 2
        for column in range(4):
            side = column // 2
            here = row * 4 + column
            for table, block in ((own, column), (other, column ^ 1)):
                if (block, earlier) in HELD[side] and block // 2 == side:
                    stage, base, parts = HELD[side][block, earlier]
                    for part in parts:
                        table[part, here] = slot_of((stage, base + part, piece))
            if side == 0 and (3, earlier) in HELD[0]:
                stage, base, parts = HELD[0][3, earlier]
                for part in parts:
                    cross[part, here] = slot_of((stage, base + part, piece))
    crossing = []
    for part in range(PARTS):
        rows = [r for r in range(row_count) if (3, r // 2) in HELD[0] and part in HELD[0][3, r // 2][2]]
        crossing.append([(r * 4 + 2 + core, r * 4 + core) for r in rows for core in range(2)])
    return send, arrive, pairs, own, other, cross, crossing, last


def ringed(slab, factor, block_inverse, pivot_order, row_count, *, sizes):
    row_indices, column_count = sizes
    _, width = slab.shape
    half = width // 2
    chunk_rows = half // PARTS
    total_width = width * column_count
    row = lax.axis_index("rows")
    column = lax.axis_index("cols")
    here = row * column_count + column
    send, arrive, pairs, own, other, cross, crossing, _ = plan(row_indices)
    steps = len(pairs)
    device = here.astype(jnp.int32)[None]

    everyone = [(r, c) for r in range(row_indices) for c in range(column_count)]

    def move(value, of):
        found = [(r * column_count + c, r * column_count + of(c)) for r, c in everyone if of(c) is not None]
        return lax.ppermute(value, AXES, found)

    def swap_core(value):
        return move(value, lambda c: c ^ 1)

    def swap_side(value):
        return move(value, lambda c: c ^ 2)

    far = swap_side(slab)
    yours = swap_core(other_half(device, factor, half))
    store, *pieces = first_chunks(device, factor, yours, own, other, half, chunk_rows)
    near = swap_core(slab)
    crossed = [None] * PARTS
    crossed[0] = lax.ppermute(pieces[0], AXES, crossing[0])

    chosen = lax.dynamic_slice_in_dim(pivot_order, column * width, width)
    index = ((chosen // width) ^ column) * width + chosen % width

    def stage_term(vectors, stage):
        return (vectors, STARTS[stage], SIZES[stage], PARTS, 0)

    def extra_term(vectors, count, first):
        return (vectors, STARTS[1] + PARTS, SIZES[1], count, first)

    def halves(which, mine, yours):
        return (mine, yours) if which % 2 else (yours, mine)

    def tied(store, *values):
        return lax.optimization_barrier((store, values))

    st = types.SimpleNamespace()
    tasks = {}

    def at(step):
        return lambda task: tasks.setdefault(step, []).append(task)

    for part in range(1, PARTS):

        @at(CROSS_SENT[part])
        def _(store, part=part):
            store, (piece,) = tied(store, pieces[part])
            crossed[part] = lax.ppermute(piece, AXES, crossing[part])
            return store

    @at(SWAP_FAR)
    def _(store):
        store, (st.far,) = tied(store, far)
        st.far_near = swap_core(st.far)
        return store

    @at(ORDER)
    def _(store):
        store, slabs = tied(store, slab, near, st.far, st.far_near)
        st.ordered = pick_columns(device, index, row_count, slabs)
        return tied(store, st.ordered)[0]

    @at(V0)
    def _(store):
        store, (ordered,) = tied(store, st.ordered)
        v0 = finish(device, 0, ordered, block_inverse)
        st.v0 = {0: v0, 1: move(v0, lambda c: {0: 1}.get(c)), 2: move(v0, lambda c: {0: 2}.get(c))}
        return tied(store, v0)[0]

    @at(PASS_0)
    def _(store):
        store, (st.v0[2],) = tied(store, st.v0[2])
        st.v0[3] = move(st.v0[2], lambda c: {2: 3}.get(c))
        return store

    @at(STAGE_0)
    def _(store):
        store, (st.v0,) = tied(store, st.v0)
        st.part = product(device, store, [stage_term(st.v0, 0)])
        st.part_near = swap_core(st.part)
        return tied(store, st.part)[0]

    @at(V1)
    def _(store):
        store, (update,) = tied(store, halves(1, st.part, st.part_near))
        v1 = finish(device, 1, st.ordered, block_inverse, [update])
        st.v1 = {1: v1, 3: move(v1, lambda c: {1: 3}.get(c))}
        if MOVED < PARTS:
            st.v1[0] = move(v1, lambda c: {1: 0}.get(c))
        return tied(store, v1)[0]

    @at(PASS_1)
    def _(store):
        store, (st.v1[3],) = tied(store, st.v1[3])
        st.v1[2] = move(st.v1[3], lambda c: {3: 2}.get(c))
        return store

    @at(STAGE_1)
    def _(store):
        store, (st.v1, part) = tied(store, st.v1, st.part)
        vectors = {c: st.v1[c] for c in (2, 3)}
        st.part = product(device, store, [stage_term(vectors, 1)], 1, part)
        st.part_near = move(st.part, lambda c: {3: 2}.get(c))
        return tied(store, st.part)[0]

    @at(V2)
    def _(store):
        store, (update,) = tied(store, halves(2, st.part, st.part_near))
        v2 = finish(device, 2, st.ordered, block_inverse, [update])
        st.v2 = {2: v2, 3: move(v2, lambda c: {2: 3}.get(c))}
        return tied(store, v2)[0]

    @at(CARRY)
    def _(store):
        terms = [stage_term({c: st.v0[c] for c in (0, 1)}, 2)]
        if MOVED < PARTS:
            terms.append(extra_term({c: st.v1[c] for c in (0, 1)}, PARTS - MOVED, 0))
        carried = product(device, store, terms, 0)
        st.carried = (move(carried, lambda c: {1: 3}.get(c)), move(carried, lambda c: {0: 3}.get(c)))
        return tied(store, carried)[0]

    arrived = [None] * steps
    for step in range(steps + DEPTH):
        values, tables = [], []
        if step >= DEPTH:
            values.append(arrived[step - DEPTH])
            tables.append(arrive[step - DEPTH])
        for part in range(PARTS):
            if CROSS_AT[part] == step:
                values.append(crossed[part])
                tables.append(cross[part])
        store, outgoing = hop(device, store, values, tables, send[step] if step < steps else None)
        if step < steps:
            arrived[step] = lax.ppermute(outgoing, AXES, pairs[step])
        for task in tasks.get(step, ()):
            store = task(store)

    terms = [stage_term(st.v2, 2), extra_term({c: st.v1[c] for c in (2, 3)}, MOVED, PARTS - MOVED)]
    part = product(device, store, terms, 1)
    updates = [halves(3, part, move(part, lambda c: {2: 3}.get(c))), st.carried]
    done = {0: st.v0[0], 1: st.v1[1], 2: st.v2[2]}
    vectors = finish(device, 3, st.ordered, block_inverse, updates, done)
    row_sums = lax.psum(jnp.sum(vectors * vectors, axis=1), "cols")
    return (vectors, row_sums / total_width)


def gathered(slab, factor, block_inverse, pivot_order, row_count):
    rows_here = slab.shape[0]
    block_width = slab.shape[1]
    column_count = lax.axis_size("cols")
    column = lax.axis_index("cols")
    total_width = block_width * column_count
    chosen = lax.dynamic_slice_in_dim(pivot_order, column * block_width, block_width)
    everything = lax.all_gather(slab, "cols", axis=1, tiled=True)
    ordered = jnp.take(everything, chosen, axis=1)
    live_rows = jnp.arange(rows_here, dtype=jnp.int32) < row_count[0]
    ordered = jnp.where(live_rows[:, None], ordered, jnp.float32(0.0))
    factor_row = lax.all_gather(factor, "rows", axis=1, tiled=True)

    def finish(values):
        return times_transposed(values, block_inverse)

    pending = ordered
    vectors = jnp.zeros_like(ordered)
    for column_block in range(column_count):
        finished = lax.cond(column == column_block, finish, jnp.zeros_like, pending)
        vectors = vectors + finished
        if column_block + 1 < column_count:
            arrived = lax.psum(finished, "cols")
            weights = factor_row[:, column_block * block_width : (column_block + 1) * block_width]
            update = times_transposed(arrived, weights)
            pending = pending - jnp.where(column_block < column, update, jnp.float32(0.0))
    row_sums = lax.psum(jnp.sum(vectors * vectors, axis=1), "cols")
    return (vectors, row_sums / total_width)


def solution(mesh):
    placed = (P("rows", "cols"), P("cols", "rows"), P("cols", None), P(), P("rows"))
    row_indices, column_count = mesh.shape["rows"], mesh.shape["cols"]
    ring = row_indices == 2 * column_count and column_count == 4

    def work(*arrays):
        if not ring:
            return gathered(*arrays)
        return ringed(*arrays, sizes=(row_indices, column_count))

    return jax.shard_map(
        work,
        mesh=mesh,
        in_specs=placed,
        out_specs=(P("rows", "cols"), P("rows")),
        check_vma=False,
    )
```
